32 devices in a mesh: dp: 8 (over y, x, core), vocab: 4 (over z).
Axes of the slice: x: 2, y: 2, z: 4, core: 2. Of those that a mesh axis runs over, the one named last changes fastest.
Arguments:
- hidden: bfloat16 [64, 4096], P('dp'), may hold values from -16 to 16
- embed_grad: bfloat16 [64, 4096], P('dp'), may hold values from -3 to 3
- token_ids: int32 [64], P('dp'), may hold values from 0 to 32767
- loss_weight: float32 [64], P('dp'), may hold values from 16 to 256
- teacher_logits: bfloat16 [64, 32768], P('dp', 'vocab'), may hold values from -24 to 256
- head: bfloat16 [4096, 32768], P('dp', 'vocab'), may hold values from -1 to 1
Outputs:
- grad_hidden: bfloat16 [64, 4096], P('dp', 'vocab')
- head_grad: float32 [4096, 32768], P('dp', 'vocab')
The draws below stay inside these ranges and needn't reach their ends.
Inputs may be any that keep to these rules, and one draw needn't show every extreme that they name: `token_ids`: token ids of the vocabulary window.
All inputs are finite; a program needn't handle non-finite values.
Results may differ from the reference program's by a relative error of at most 0.0022.
The reference program's roundings to bfloat16 on the way (of `gap`) count: a program that leaves them out, or rounds other values in their place, can miss the bound.
Values may be sent and summed in bfloat16 or wider, within the bound.
A program may use at most 128 MiB of HBM per device.

```python
import math
import jax
import jax.numpy as jnp
import numpy as np
from jax import lax

D = 4096
TOKENS = 64
VOCAB_WIN = 32768


def head_values(key):
    raw = jax.random.normal(jax.random.fold_in(key, 11), (D, VOCAB_WIN), jnp.float32)
    return jnp.clip(raw * (3.0 / math.sqrt(D)), -1.0, 1.0)


def draw_head(key, part):
    return head_values(key).astype(jnp.bfloat16)


def draw_hidden(key, part):
    base = jax.random.normal(jax.random.fold_in(key, 23), (TOKENS, D), jnp.float32)
    return jnp.clip(base, -16.0, 16.0).astype(jnp.bfloat16)


def draw_teacher_logits(key, part):
    base = jax.random.normal(jax.random.fold_in(key, 53), (TOKENS, VOCAB_WIN), jnp.float32) * 3.0
    return jnp.clip(base, -24.0, 256.0).astype(jnp.bfloat16)


def place_ends(values, stream_key, smallest, top_value):
    dims = values.shape
    index_at = [jax.random.randint(jax.random.fold_in(stream_key, axis), (), 0, dims[axis]) for axis in range(len(dims))]
    values = values.at[tuple(index_at)].set(smallest)
    longest = dims.index(max(dims))
    index_at[longest] = (index_at[longest] + 1) % dims[longest]
    return values.at[tuple(index_at)].set(top_value)


def with_spikes(result, rng, source, target, blocks, factor):
    def block_of(axis_at):
        return (jnp.arange(result.shape[axis_at]) // (result.shape[axis_at] // blocks)).reshape((-1,) + (1,) * (result.ndim - 1 - axis_at))

    one_side = jax.random.permutation(rng, blocks)[block_of(target)]
    second = (block_of(target) + blocks // 2) % blocks
    return jnp.where((block_of(source) == one_side) | (block_of(source) == second), factor * result, result)


def shard_levels(own_key, dims, split, low, top_value):
    factor_of, own = 1.0, jax.random.fold_in(own_key, 6)
    for dim, blocks in split:
        heights = jnp.exp(jax.random.uniform(jax.random.fold_in(own, dim), (blocks,), jnp.float32, low / len(split), top_value / len(split)))
        factor_of = factor_of * jnp.repeat(heights, dims[dim] // blocks).reshape([-1 if axis == dim else 1 for axis in range(len(dims))])
    return factor_of


def cumulative_ranks(amount, lean):
    loads = [(1 << 20) // math.isqrt(grade ** lean) + 1 for grade in range(1, amount + 1)]
    width = 1 + sum(loads) // (1 << 30)
    return np.cumsum(np.array([max(1, weight // width) for weight in loads]))


def ranked_ids(stream_key, dims, amount, slope):
    table = cumulative_ranks(amount, slope)
    ticket = jax.random.randint(jax.random.fold_in(stream_key, 1), dims, 0, int(table[amount - 1]))
    rank = jnp.searchsorted(jnp.asarray(table, jnp.int32), ticket, side="right")
    return jax.random.permutation(jax.random.fold_in(stream_key, 2), amount)[rank].astype(jnp.int32)


def bell_draw_with(key, extent, deviation, most, shards, heavy, kind=jnp.bfloat16):
    drawn = deviation * jax.random.normal(key, extent, jnp.float32)
    if shards:
        drawn = drawn * shard_levels(key, extent, shards, -0.22, 0.18)
    return jnp.clip(with_spikes(drawn, jax.random.fold_in(key, 3), *heavy), -most, most).astype(kind)


def setup_inputs(seed: int = 0) -> dict:
    streams_of = jax.random.split(jax.random.key(seed), 7)
    return {
        "hidden": draw_hidden(jax.random.fold_in(streams_of[6], 71), 0),
        "embed_grad": bell_draw_with(streams_of[1], (TOKENS, D), 0.5, 3.0, ((0, 8),), (0, 1, 8, 2.0)),
        "token_ids": place_ends(ranked_ids(streams_of[2], (TOKENS,), VOCAB_WIN, 2), jax.random.fold_in(streams_of[2], 3), 0, VOCAB_WIN - 1).astype(jnp.int32),
        "loss_weight": jnp.clip(jnp.exp(math.log(256.0) - 2.7725887 * jax.random.uniform(streams_of[3], (TOKENS,), jnp.float32) ** shard_levels(streams_of[3], (TOKENS,), ((0, 8),), -0.2, 0.2)), 16.0, 256.0),
        "teacher_logits": draw_teacher_logits(jax.random.fold_in(streams_of[6], 71), 0),
        "head": draw_head(jax.random.fold_in(streams_of[6], 71), 0),
    }


def reference(hidden, embed_grad, token_ids, loss_weight, teacher_logits, head):
    student = jnp.dot(hidden, head, preferred_element_type=jnp.float32)
    teacher = teacher_logits.astype(jnp.float32)
    student_norm = jax.nn.logsumexp(student, axis=1, keepdims=True)
    teacher_norm = jax.nn.logsumexp(teacher, axis=1, keepdims=True)
    gap = (loss_weight[:, None] * (jnp.exp(student - student_norm) - jnp.exp(teacher - teacher_norm))).astype(jnp.bfloat16)
    dense_part = lax.dot_general(hidden, gap, (((0,), (0,)), ((), ())), preferred_element_type=jnp.float32)
    head_grad = dense_part.at[:, token_ids.astype(jnp.int32)].add(embed_grad.astype(jnp.float32).T)
    grad_hidden = lax.dot_general(gap, head, (((1,), (1,)), ((), ())), preferred_element_type=jnp.float32).astype(jnp.bfloat16)
    return grad_hidden, head_grad
```

```python
import functools

import jax
import jax.numpy as jnp
from jax import lax
from jax.experimental import pallas as pl
from jax.experimental.pallas import tpu as pltpu
from jax.sharding import PartitionSpec as P

MESH = pl.DeviceIdType.MESH
F32 = jnp.float32
BF16 = jnp.bfloat16


def flat_rows(block):
    return block.astype(F32).reshape(block.shape[0] * block.shape[1], block.shape[2]).astype(BF16)


def comm_kernel(
    n, nv, chunks, pieces,
    hidden, embed, ids, weight, teacher, head,
    grad_out, gap_out, hid_out, emb_out, ids_out,
    hc, ec, idt, tea, head_v, hx, part, xbuf, total, rsbuf, stu, stat, ga, bk, fin,
    head_sem, tea_sem, own_sem, out_sem,
    hid_s, hid_r, emb_s, emb_r, ids_s, ids_r,
    pair_s, pair_r, rs_s, rs_r, st_s, st_r, ag_s, ag_r, fw_s, fw_r, fin_s, fin_r,
):
    i = lax.axis_index("dp")
    v = lax.axis_index("vocab")
    nc = n // 2
    core = lax.rem(i, 2)
    chip = lax.div(i, 2)
    partner = i + 1 - 2 * core
    rows, vocab = teacher.shape
    width = vocab // chunks
    cut = vocab // pieces
    group = n // nv

    def slot(j):
        return lax.rem(j, 2) * nc + lax.div(j, 2)

    mine = slot(i)

    def remote(src, dst, send, recv, dp, vo=None):
        return pltpu.make_async_remote_copy(
            src_ref=src, dst_ref=dst, send_sem=send, recv_sem=recv,
            device_id=(dp, v if vo is None else vo), device_id_type=MESH,
        )

    barrier = pltpu.get_barrier_semaphore()
    for dd in range(n):
        for dv in range(nv):
            if dd or dv:
                pl.semaphore_signal(
                    barrier, inc=1,
                    device_id=(lax.rem(i + dd, n), lax.rem(v + dv, nv)),
                    device_id_type=MESH,
                )

    own = [
        pltpu.make_async_copy(hidden.at[i], hc.at[mine], own_sem.at[0]),
        pltpu.make_async_copy(embed.at[i], ec.at[mine], own_sem.at[1]),
    ]
    for copy in own:
        copy.start()
    heads = []
    for ch in range(chunks):
        cols = pl.ds(ch * width, width)
        heads.append(pltpu.make_async_copy(head.at[:, cols], head_v.at[:, cols], head_sem.at[ch]))
        heads[-1].start()
    tea_copy = pltpu.make_async_copy(teacher, tea, tea_sem)
    tea_copy.start()

    row = lax.broadcasted_iota(jnp.int32, (rows, 128), 0)
    id_tile = jnp.zeros((rows, 128), jnp.int32)
    w_tile = jnp.zeros((rows, 128), F32)
    for r in range(rows):
        id_tile = jnp.where(row == r, ids[r], id_tile)
        w_tile = jnp.where(row == r, weight[r], w_tile)
    idt[mine] = id_tile
    w_col = w_tile[:, 0:1]

    pl.semaphore_wait(barrier, n * nv - 1)

    hid, emb, idc = [], [], []
    for d in range(1, n):
        j = lax.rem(i + d, n)
        hid.append(remote(hidden.at[j], hc.at[mine], hid_s.at[d], hid_r.at[d], j))
        hid[-1].start()
    for d in range(1, n):
        j = lax.rem(i + d, n)
        emb.append(remote(embed.at[j], ec.at[mine], emb_s.at[d], emb_r.at[d], j))
        idc.append(remote(idt.at[mine], idt.at[mine], ids_s.at[d], ids_r.at[d], j))
        emb[-1].start()
        idc[-1].start()

    own[0].wait()
    for copy in hid:
        copy.wait_recv()
    hx[...] = flat_rows(hc[...])
    hid_copy = pltpu.make_async_copy(hc, hid_out, out_sem.at[0])
    hid_copy.start()

    pair, rs = [], []

    def reduce_pair(ch):
        pair[ch].wait_recv()
        total[ch] = part[ch, core] + xbuf[ch]
        sends = []
        for d in range(1, nc):
            k = lax.rem(chip + d, nc)
            sends.append(
                remote(total.at[ch, k], rsbuf.at[ch, d], rs_s.at[ch, d], rs_r.at[ch, d], 2 * k + core)
            )
            sends[-1].start()
        rs.append(sends)

    for ch in range(chunks):
        heads[ch].wait()
        product = jnp.dot(
            hx[...], head_v[:, ch * width:(ch + 1) * width], preferred_element_type=F32
        )
        part[ch] = product.reshape(2, nc, rows, width)
        pair.append(remote(part.at[ch, 1 - core], xbuf.at[ch], pair_s.at[ch], pair_r.at[ch], partner))
        pair[ch].start()
        if ch:
            reduce_pair(ch - 1)
    reduce_pair(chunks - 1)

    tea_copy.wait()
    t = tea[...].astype(F32)
    t_max = jnp.max(t, axis=1, keepdims=True)
    t_sum = jnp.sum(jnp.exp(t - t_max), axis=1, keepdims=True)

    own[1].wait()
    for copy in emb + idc:
        copy.wait_recv()
    emb_copy = pltpu.make_async_copy(ec, emb_out, out_sem.at[1])
    ids_copy = pltpu.make_async_copy(idt, ids_out, out_sem.at[2])
    emb_copy.start()
    ids_copy.start()

    s_max = None
    for ch in range(chunks):
        s = total[ch, chip]
        for d in range(1, nc):
            rs[ch][d - 1].wait_recv()
            s = s + rsbuf[ch, d]
        stu[:, ch * width:(ch + 1) * width] = s
        top = jnp.max(s, axis=1, keepdims=True)
        s_max = top if s_max is None else jnp.maximum(s_max, top)
    s_sum = jnp.sum(jnp.exp(stu[...] - s_max), axis=1, keepdims=True)

    lane = lax.broadcasted_iota(jnp.int32, (rows, 128), 1)
    stat[0] = jnp.where(
        lane == 0, s_max, jnp.where(lane == 1, s_sum, jnp.where(lane == 2, t_max, t_sum))
    )
    sts = []
    for d in range(1, nv):
        sts.append(
            remote(stat.at[0], stat.at[d], st_s.at[d], st_r.at[d], i, lax.rem(v + d, nv))
        )
        sts[-1].start()
    for copy in sts:
        copy.wait_recv()
    s_tops = [stat[d][:, 0:1] for d in range(nv)]
    t_tops = [stat[d][:, 2:3] for d in range(nv)]
    s_top = functools.reduce(jnp.maximum, s_tops)
    t_top = functools.reduce(jnp.maximum, t_tops)
    s_tot = sum(stat[d][:, 1:2] * jnp.exp(s_tops[d] - s_top) for d in range(nv))
    t_tot = sum(stat[d][:, 3:4] * jnp.exp(t_tops[d] - t_top) for d in range(nv))
    s_norm = s_top + jnp.log(s_tot)
    t_norm = t_top + jnp.log(t_tot)

    ag, fw = [], []
    for g in range(pieces):
        cols = pl.ds(g * cut, cut)
        gap = w_col * (
            jnp.exp(stu[:, cols] - s_norm) - jnp.exp(tea[:, cols].astype(F32) - t_norm)
        )
        ga[mine, :, cols] = gap.astype(BF16)
        block = ga.at[mine, :, cols]
        sends = []
        for d in range(1, nc):
            k = lax.rem(chip + d, nc)
            sends.append(remote(block, block, ag_s.at[g, d], ag_r.at[g, d], 2 * k + core))
            sends[-1].start()
        ag.append(sends)
        fw.append([remote(block, block, fw_s.at[g, 0], fw_r.at[g, 0], partner)])
        fw[g][0].start()

    back = jnp.zeros(hx.shape, F32)
    for g in range(pieces):
        cols = pl.ds(g * cut, cut)
        for d in range(1, nc):
            ag[g][d - 1].wait_recv()
            k = lax.rem(chip + nc - d, nc)
            block = ga.at[core * nc + k, :, cols]
            fw[g].append(remote(block, block, fw_s.at[g, d], fw_r.at[g, d], partner))
            fw[g][d].start()
        for copy in fw[g]:
            copy.wait_recv()
        back = back + lax.dot_general(
            flat_rows(ga[:, :, cols]), head_v[:, g * cut:(g + 1) * cut],
            (((1,), (1,)), ((), ())), preferred_element_type=F32,
        )
    gap_copy = pltpu.make_async_copy(ga, gap_out, out_sem.at[3])
    gap_copy.start()
    bk[...] = back.reshape(bk.shape)

    dest = lax.div(i, group)
    source = lax.rem(i, group) * nv + v
    fins = []
    for d in range(n):
        j = lax.rem(i + d, n)
        fins.append(
            remote(bk.at[slot(j)], fin.at[source], fin_s.at[d], fin_r.at[source], j, dest)
        )
    stays = dest == v
    self_copy = pltpu.make_async_copy(bk.at[mine], fin.at[source], fin_r.at[source])
    for d in range(1, n):
        fins[d].start()

    @pl.when(stays)
    def _():
        self_copy.start()

    @pl.when(jnp.logical_not(stays))
    def _():
        fins[0].start()

    for q in range(n):
        pltpu.make_async_copy(fin.at[q], fin.at[q], fin_r.at[q]).wait()
    wide = hx.shape[1]
    for r in range(group):
        grad = fin[r * nv]
        for q in range(1, nv):
            grad = grad + fin[r * nv + q]
        grad_out[:, r * wide:(r + 1) * wide] = grad.astype(BF16)

    for copy in hid + emb + idc + pair + sts + fins[1:]:
        copy.wait_send()
    for sends in rs + ag + fw:
        for copy in sends:
            copy.wait_send()

    @pl.when(jnp.logical_not(stays))
    def _():
        fins[0].wait_send()

    hid_copy.wait()
    emb_copy.wait()
    ids_copy.wait()
    gap_copy.wait()


def head_grad_kernel(hid, emb, ids, gap, out, lhs):
    step = pl.program_id(0)
    tokens = hid.shape[0] * hid.shape[1]
    width = out.shape[1]

    @pl.when(step == 0)
    def _():
        both = jnp.concatenate(
            [a[...].astype(F32).reshape(tokens, a.shape[2]) for a in (hid, emb)], axis=0
        )
        lhs[...] = both.T.astype(BF16)

    first = (lax.axis_index("vocab") * pl.num_programs(0) + step) * width
    column = lax.broadcasted_iota(jnp.int32, (tokens, width), 1) + first
    token = ids[...].reshape(tokens, ids.shape[2])[:, 0:1]
    lookup = jnp.where(column == token, 1.0, 0.0)
    rhs = jnp.concatenate([gap[...].astype(F32).reshape(tokens, width), lookup], axis=0)
    out[...] = jnp.dot(lhs[...], rhs.astype(BF16), preferred_element_type=F32)


def per_device(n, nv, hidden, embed_grad, token_ids, loss_weight, teacher_logits, head):
    rows, model = hidden.shape
    wide, vocab = head.shape
    nc = n // 2
    chunks = 8 if n <= 8 else 4
    pieces = 4
    tokens = n * rows

    def blocks(a):
        return a.reshape(rows, n, wide).swapaxes(0, 1)

    dma = pltpu.SemaphoreType.DMA
    any_spec = pl.BlockSpec(memory_space=pl.ANY)
    vmem_spec = pl.BlockSpec(memory_space=pltpu.VMEM)
    smem_spec = pl.BlockSpec(memory_space=pltpu.SMEM)
    grad_hidden, gap, hid, emb, ids = pl.pallas_call(
        functools.partial(comm_kernel, n, nv, chunks, pieces),
        out_shape=(
            jax.ShapeDtypeStruct((rows, model // nv), BF16),
            jax.ShapeDtypeStruct((n, rows, vocab), BF16),
            jax.ShapeDtypeStruct((n, rows, wide), BF16),
            jax.ShapeDtypeStruct((n, rows, wide), BF16),
            jax.ShapeDtypeStruct((n, rows, 128), jnp.int32),
        ),
        in_specs=[any_spec, any_spec, smem_spec, smem_spec, any_spec, any_spec],
        out_specs=(vmem_spec, any_spec, any_spec, any_spec, any_spec),
        scratch_shapes=[
            pltpu.VMEM((n, rows, wide), BF16),
            pltpu.VMEM((n, rows, wide), BF16),
            pltpu.VMEM((n, rows, 128), jnp.int32),
            pltpu.VMEM((rows, vocab), BF16),
            pltpu.VMEM((wide, vocab), BF16),
            pltpu.VMEM((tokens, wide), BF16),
            pltpu.VMEM((chunks, 2, nc, rows, vocab // chunks), F32),
            pltpu.VMEM((chunks, nc, rows, vocab // chunks), F32),
            pltpu.VMEM((chunks, nc, rows, vocab // chunks), F32),
            pltpu.VMEM((chunks, nc, rows, vocab // chunks), F32),
            pltpu.VMEM((rows, vocab), F32),
            pltpu.VMEM((nv, rows, 128), F32),
            pltpu.VMEM((n, rows, vocab), BF16),
            pltpu.VMEM((n, rows, wide), F32),
            pltpu.VMEM((n, rows, wide), F32),
            dma((chunks,)), dma, dma((2,)), dma((4,)),
            dma((n,)), dma((n,)), dma((n,)), dma((n,)), dma((n,)), dma((n,)),
            dma((chunks,)), dma((chunks,)),
            dma((chunks, nc)), dma((chunks, nc)),
            dma((nv,)), dma((nv,)),
            dma((pieces, nc)), dma((pieces, nc)), dma((pieces, nc)), dma((pieces, nc)),
            dma((n,)), dma((n,)),
        ],
        compiler_params=pltpu.CompilerParams(
            collective_id=0, has_side_effects=True, vmem_limit_bytes=64_000_000
        ),
        name="exchange",
    )(blocks(hidden), blocks(embed_grad), token_ids, loss_weight, teacher_logits, head)

    steps = 8
    cols = vocab // steps
    head_grad = pl.pallas_call(
        head_grad_kernel,
        grid=(steps,),
        out_shape=jax.ShapeDtypeStruct((wide, vocab), F32),
        in_specs=[
            pl.BlockSpec((n, rows, wide), lambda s: (0, 0, 0)),
            pl.BlockSpec((n, rows, wide), lambda s: (0, 0, 0)),
            pl.BlockSpec((n, rows, 128), lambda s: (0, 0, 0)),
            pl.BlockSpec((n, rows, cols), lambda s: (0, 0, s)),
        ],
        out_specs=pl.BlockSpec((wide, cols), lambda s: (0, s)),
        scratch_shapes=[pltpu.VMEM((wide, 2 * tokens), BF16)],
        compiler_params=pltpu.CompilerParams(vmem_limit_bytes=40_000_000),
        name="head_grad",
    )(hid, emb, ids, gap)
    return grad_hidden, head_grad


def solution(mesh):
    placed = (P("dp", None), P("dp", None), P("dp"), P("dp"), P("dp", "vocab"), P("dp", "vocab"))
    return jax.shard_map(
        functools.partial(per_device, mesh.shape["dp"], mesh.shape["vocab"]),
        mesh=mesh,
        in_specs=placed,
        out_specs=(P("dp", "vocab"), P("dp", "vocab")),
        check_vma=False,
    )
```

```python
import functools

import jax
import jax.numpy as jnp
from jax import lax
from jax.experimental import pallas as pl
from jax.experimental.pallas import tpu as pltpu
from jax.sharding import PartitionSpec as P

MESH = pl.DeviceIdType.MESH
F32 = jnp.float32
BF16 = jnp.bfloat16


def flat_rows(block):
    return block.astype(F32).reshape(block.shape[0] * block.shape[1], block.shape[2]).astype(BF16)


def comm_kernel(
    n, nv, chunks, pieces,
    hidden, embed, ids, weight, teacher, head,
    grad_out, gap_out, hid_out, emb_out, ids_out,
    hc, ec, idt, tea, head_v, hx, part, xbuf, total, rsbuf, stu, stat, ga, bk, bq, fin,
    head_sem, tea_sem, own_sem, out_sem,
    hid_s, hid_r, emb_s, emb_r, ids_s, ids_r,
    pair_s, pair_r, rs_s, rs_r, st_s, st_r, ag_s, ag_r, fw_s, fw_r, row_s, row_r, fin_s, fin_r,
):
    i = lax.axis_index("dp")
    v = lax.axis_index("vocab")
    nc = n // 2
    core = lax.rem(i, 2)
    chip = lax.div(i, 2)
    partner = i + 1 - 2 * core
    rows, vocab = teacher.shape
    width = vocab // chunks
    cut = vocab // pieces
    group = n // nv

    def slot(j):
        return lax.rem(j, 2) * nc + lax.div(j, 2)

    mine = slot(i)

    def remote(src, dst, send, recv, dp, vo=None):
        return pltpu.make_async_remote_copy(
            src_ref=src, dst_ref=dst, send_sem=send, recv_sem=recv,
            device_id=(dp, v if vo is None else vo), device_id_type=MESH,
        )

    barrier = pltpu.get_barrier_semaphore()
    peers = [(lax.rem(i + d, n), v) for d in range(1, n)]
    peers += [(i, lax.rem(v + d, nv)) for d in range(1, nv)]
    for peer in peers:
        pl.semaphore_signal(barrier, inc=1, device_id=peer, device_id_type=MESH)

    own = [
        pltpu.make_async_copy(hidden.at[i], hc.at[mine], own_sem.at[0]),
        pltpu.make_async_copy(embed.at[i], ec.at[mine], own_sem.at[1]),
    ]
    for copy in own:
        copy.start()
    heads = []
    for ch in range(chunks):
        cols = pl.ds(ch * width, width)
        heads.append(pltpu.make_async_copy(head.at[:, cols], head_v.at[:, cols], head_sem.at[ch]))
        heads[-1].start()
    tea_copy = pltpu.make_async_copy(teacher, tea, tea_sem)
    tea_copy.start()

    row = lax.broadcasted_iota(jnp.int32, (rows, 128), 0)
    id_tile = jnp.zeros((rows, 128), jnp.int32)
    w_tile = jnp.zeros((rows, 128), F32)
    for r in range(rows):
        id_tile = jnp.where(row == r, ids[r], id_tile)
        w_tile = jnp.where(row == r, weight[r], w_tile)
    idt[mine] = id_tile
    w_col = w_tile[:, 0:1]

    pl.semaphore_wait(barrier, len(peers))

    hid, emb, idc = [], [], []
    for d in range(1, n):
        j = lax.rem(i + d, n)
        hid.append(remote(hidden.at[j], hc.at[mine], hid_s.at[d], hid_r.at[d], j))
        hid[-1].start()
    for d in range(1, n):
        j = lax.rem(i + d, n)
        emb.append(remote(embed.at[j], ec.at[mine], emb_s.at[d], emb_r.at[d], j))
        idc.append(remote(idt.at[mine], idt.at[mine], ids_s.at[d], ids_r.at[d], j))
        emb[-1].start()
        idc[-1].start()

    own[0].wait()
    for copy in hid:
        copy.wait_recv()
    hx[...] = flat_rows(hc[...])
    hid_copy = pltpu.make_async_copy(hc, hid_out, out_sem.at[0])
    hid_copy.start()

    pair, rs = [], []

    def reduce_pair(ch):
        pair[ch].wait_recv()
        total[ch] = part[ch, core] + xbuf[ch]
        sends = []
        for d in range(1, nc):
            k = lax.rem(chip + d, nc)
            sends.append(
                remote(total.at[ch, k], rsbuf.at[ch, d], rs_s.at[ch, d], rs_r.at[ch, d], 2 * k + core)
            )
            sends[-1].start()
        rs.append(sends)

    for ch in range(chunks):
        heads[ch].wait()
        product = jnp.dot(
            hx[...], head_v[:, ch * width:(ch + 1) * width], preferred_element_type=F32
        )
        part[ch] = product.reshape(2, nc, rows, width)
        pair.append(remote(part.at[ch, 1 - core], xbuf.at[ch], pair_s.at[ch], pair_r.at[ch], partner))
        pair[ch].start()
        if ch:
            reduce_pair(ch - 1)
    reduce_pair(chunks - 1)

    tea_copy.wait()
    t = tea[...].astype(F32)
    t_max = jnp.max(t, axis=1, keepdims=True)
    t_sum = jnp.sum(jnp.exp(t - t_max), axis=1, keepdims=True)

    own[1].wait()
    for copy in emb + idc:
        copy.wait_recv()
    emb_copy = pltpu.make_async_copy(ec, emb_out, out_sem.at[1])
    ids_copy = pltpu.make_async_copy(idt, ids_out, out_sem.at[2])
    emb_copy.start()
    ids_copy.start()

    s_max = None
    for ch in range(chunks):
        s = total[ch, chip]
        for d in range(1, nc):
            rs[ch][d - 1].wait_recv()
            s = s + rsbuf[ch, d]
        stu[:, ch * width:(ch + 1) * width] = s
        top = jnp.max(s, axis=1, keepdims=True)
        s_max = top if s_max is None else jnp.maximum(s_max, top)
    s_sum = jnp.sum(jnp.exp(stu[...] - s_max), axis=1, keepdims=True)

    lane = lax.broadcasted_iota(jnp.int32, (rows, 128), 1)
    stat[0] = jnp.where(
        lane == 0, s_max, jnp.where(lane == 1, s_sum, jnp.where(lane == 2, t_max, t_sum))
    )
    sts = []
    for d in range(1, nv):
        sts.append(
            remote(stat.at[0], stat.at[d], st_s.at[d], st_r.at[d], i, lax.rem(v + d, nv))
        )
        sts[-1].start()
    for copy in sts:
        copy.wait_recv()
    s_tops = [stat[d][:, 0:1] for d in range(nv)]
    t_tops = [stat[d][:, 2:3] for d in range(nv)]
    s_top = functools.reduce(jnp.maximum, s_tops)
    t_top = functools.reduce(jnp.maximum, t_tops)
    s_tot = sum(stat[d][:, 1:2] * jnp.exp(s_tops[d] - s_top) for d in range(nv))
    t_tot = sum(stat[d][:, 3:4] * jnp.exp(t_tops[d] - t_top) for d in range(nv))
    s_norm = s_top + jnp.log(s_tot)
    t_norm = t_top + jnp.log(t_tot)

    ag, fw = [], []
    for g in range(pieces):
        cols = pl.ds(g * cut, cut)
        gap = w_col * (
            jnp.exp(stu[:, cols] - s_norm) - jnp.exp(tea[:, cols].astype(F32) - t_norm)
        )
        ga[mine, :, cols] = gap.astype(BF16)
        block = ga.at[mine, :, cols]
        sends = []
        for d in range(1, nc):
            k = lax.rem(chip + d, nc)
            sends.append(remote(block, block, ag_s.at[g, d], ag_r.at[g, d], 2 * k + core))
            sends[-1].start()
        ag.append(sends)
        fw.append([remote(block, block, fw_s.at[g, 0], fw_r.at[g, 0], partner)])
        fw[g][0].start()

    back = jnp.zeros(hx.shape, F32)
    for g in range(pieces):
        cols = pl.ds(g * cut, cut)
        for d in range(1, nc):
            ag[g][d - 1].wait_recv()
            k = lax.rem(chip + nc - d, nc)
            block = ga.at[core * nc + k, :, cols]
            fw[g].append(remote(block, block, fw_s.at[g, d], fw_r.at[g, d], partner))
            fw[g][d].start()
        for copy in fw[g]:
            copy.wait_recv()
        back = back + lax.dot_general(
            flat_rows(ga[:, :, cols]), head_v[:, g * cut:(g + 1) * cut],
            (((1,), (1,)), ((), ())), preferred_element_type=F32,
        )
    gap_copy = pltpu.make_async_copy(ga, gap_out, out_sem.at[3])
    gap_copy.start()
    bk[...] = back.reshape(bk.shape)

    self_copy = pltpu.make_async_copy(bk.at[mine], bq.at[i], row_r.at[i])
    self_copy.start()
    rows_out = []
    for d in range(1, n):
        j = lax.rem(i + d, n)
        rows_out.append(remote(bk.at[slot(j)], bq.at[i], row_s.at[d], row_r.at[i], j))
        rows_out[-1].start()
    fins = []
    for d in range(1, nv + 1):
        u = lax.rem(v + d, nv)
        for r in range(group):
            q = u * group + r
            pltpu.make_async_copy(bq.at[q], bq.at[q], row_r.at[q]).wait()
        if d < nv:
            fins.append(
                remote(bq.at[pl.ds(u * group, group)], fin.at[d], fin_s.at[d], fin_r.at[d], i, u)
            )
            fins[-1].start()
    for copy in fins:
        copy.wait_recv()
    wide = hx.shape[1]
    for r in range(group):
        grad = bq[v * group + r]
        for d in range(1, nv):
            grad = grad + fin[d, r]
        grad_out[:, r * wide:(r + 1) * wide] = grad.astype(BF16)

    for copy in hid + emb + idc + pair + sts + rows_out + fins:
        copy.wait_send()
    for sends in rs + ag + fw:
        for copy in sends:
            copy.wait_send()

    hid_copy.wait()
    emb_copy.wait()
    ids_copy.wait()
    gap_copy.wait()


def head_grad_kernel(hid, emb, ids, gap, out, lhs):
    step = pl.program_id(0)
    tokens = hid.shape[0] * hid.shape[1]
    width = out.shape[1]

    @pl.when(step == 0)
    def _():
        both = jnp.concatenate(
            [a[...].astype(F32).reshape(tokens, a.shape[2]) for a in (hid, emb)], axis=0
        )
        lhs[...] = both.T.astype(BF16)

    first = (lax.axis_index("vocab") * pl.num_programs(0) + step) * width
    column = lax.broadcasted_iota(jnp.int32, (tokens, width), 1) + first
    token = ids[...].reshape(tokens, ids.shape[2])[:, 0:1]
    lookup = jnp.where(column == token, 1.0, 0.0)
    rhs = jnp.concatenate([gap[...].astype(F32).reshape(tokens, width), lookup], axis=0)
    out[...] = jnp.dot(lhs[...], rhs.astype(BF16), preferred_element_type=F32)


def per_device(n, nv, hidden, embed_grad, token_ids, loss_weight, teacher_logits, head):
    rows, model = hidden.shape
    wide, vocab = head.shape
    nc = n // 2
    chunks = 8 if n <= 8 else 4
    pieces = 4
    tokens = n * rows

    def blocks(a):
        return a.reshape(rows, n, wide).swapaxes(0, 1)

    dma = pltpu.SemaphoreType.DMA
    any_spec = pl.BlockSpec(memory_space=pl.ANY)
    vmem_spec = pl.BlockSpec(memory_space=pltpu.VMEM)
    smem_spec = pl.BlockSpec(memory_space=pltpu.SMEM)
    grad_hidden, gap, hid, emb, ids = pl.pallas_call(
        functools.partial(comm_kernel, n, nv, chunks, pieces),
        out_shape=(
            jax.ShapeDtypeStruct((rows, model // nv), BF16),
            jax.ShapeDtypeStruct((n, rows, vocab), BF16),
            jax.ShapeDtypeStruct((n, rows, wide), BF16),
            jax.ShapeDtypeStruct((n, rows, wide), BF16),
            jax.ShapeDtypeStruct((n, rows, 128), jnp.int32),
        ),
        in_specs=[any_spec, any_spec, smem_spec, smem_spec, any_spec, any_spec],
        out_specs=(vmem_spec, any_spec, any_spec, any_spec, any_spec),
        scratch_shapes=[
            pltpu.VMEM((n, rows, wide), BF16),
            pltpu.VMEM((n, rows, wide), BF16),
            pltpu.VMEM((n, rows, 128), jnp.int32),
            pltpu.VMEM((rows, vocab), BF16),
            pltpu.VMEM((wide, vocab), BF16),
            pltpu.VMEM((tokens, wide), BF16),
            pltpu.VMEM((chunks, 2, nc, rows, vocab // chunks), F32),
            pltpu.VMEM((chunks, nc, rows, vocab // chunks), F32),
            pltpu.VMEM((chunks, nc, rows, vocab // chunks), F32),
            pltpu.VMEM((chunks, nc, rows, vocab // chunks), F32),
            pltpu.VMEM((rows, vocab), F32),
            pltpu.VMEM((nv, rows, 128), F32),
            pltpu.VMEM((n, rows, vocab), BF16),
            pltpu.VMEM((n, rows, wide), F32),
            pltpu.VMEM((n, rows, wide), F32),
            pltpu.VMEM((nv, n // nv, rows, wide), F32),
            dma((chunks,)), dma, dma((2,)), dma((4,)),
            dma((n,)), dma((n,)), dma((n,)), dma((n,)), dma((n,)), dma((n,)),
            dma((chunks,)), dma((chunks,)),
            dma((chunks, nc)), dma((chunks, nc)),
            dma((nv,)), dma((nv,)),
            dma((pieces, nc)), dma((pieces, nc)), dma((pieces, nc)), dma((pieces, nc)),
            dma((n,)), dma((n,)), dma((nv,)), dma((nv,)),
        ],
        compiler_params=pltpu.CompilerParams(
            collective_id=0, has_side_effects=True, vmem_limit_bytes=64_000_000
        ),
        name="exchange",
    )(blocks(hidden), blocks(embed_grad), token_ids, loss_weight, teacher_logits, head)

    steps = 8
    cols = vocab // steps
    head_grad = pl.pallas_call(
        head_grad_kernel,
        grid=(steps,),
        out_shape=jax.ShapeDtypeStruct((wide, vocab), F32),
        in_specs=[
            pl.BlockSpec((n, rows, wide), lambda s: (0, 0, 0)),
            pl.BlockSpec((n, rows, wide), lambda s: (0, 0, 0)),
            pl.BlockSpec((n, rows, 128), lambda s: (0, 0, 0)),
            pl.BlockSpec((n, rows, cols), lambda s: (0, 0, s)),
        ],
        out_specs=pl.BlockSpec((wide, cols), lambda s: (0, s)),
        scratch_shapes=[pltpu.VMEM((wide, 2 * tokens), BF16)],
        compiler_params=pltpu.CompilerParams(vmem_limit_bytes=64_000_000),
        name="head_grad",
    )(hid, emb, ids, gap)
    return grad_hidden, head_grad


def solution(mesh):
    placed = (P("dp", None), P("dp", None), P("dp"), P("dp"), P("dp", "vocab"), P("dp", "vocab"))
    return jax.shard_map(
        functools.partial(per_device, mesh.shape["dp"], mesh.shape["vocab"]),
        mesh=mesh,
        in_specs=placed,
        out_specs=(P("dp", "vocab"), P("dp", "vocab")),
        check_vma=False,
    )
```
